32 devices in a mesh: lat: 4 (over z), lon: 8 (over y, x, core).
Axes of the slice: x: 2, y: 2, z: 4, core: 2. Of those that a mesh axis runs over, the one named last changes fastest.
Arguments:
- fields: bfloat16 [3, 512, 32, 384], P(None, ('lat', 'lon')), may hold values from -6 to 6
- weights: bfloat16 [3, 1024, 8, 32, 128], P(None, ('lat', 'lon')), may hold values from -0.5 to 0.5
- pair_slots: int32 [3, 1024, 8], P(None, ('lat', 'lon')), may hold values from 0 to 15
- pair_counts: int32 [3, 1024], P(None, ('lat', 'lon')), may hold values from 1 to 8
- requests: int32 [3, 32, 16], replicated, may hold values from 0 to 511, as said below
- eofs: bfloat16 [200, 131072], P(None, ('lat', 'lon')), may hold values from -0.015625 to 0.015625
Outputs:
- pcs: float32 [200, 1152], P(None, ('lat', 'lon'))
The draws below stay inside these ranges and needn't reach their ends.
Inputs may be any that keep to these rules, and one draw needn't show every extreme that they name: requests[g, d] lists 16 distinct source tiles for grid g and device d (d = lat index * lon devices + lon index); source tile j lies on device j // 16; all of them lie on devices with d's lat index whose lon index is d's own or one of its two cyclic neighbours, at most 8 on any one device, and exactly 8 on some device for every g and d. `pair_slots`: only entries with p < pair_counts[g, t] are used.
All inputs are finite; a program needn't handle non-finite values.
Results may differ from the reference program's by a relative error of at most 0.0029.
Values may be sent and summed in bfloat16 or wider, within the bound.
A program may use at most 128 MiB of HBM per device.

```python
import jax
import jax.numpy as jnp
from jax import lax

EOFS = 200
TT = 128
TS = 32
MAXP = 8
MONTHS = 24
GRIDS = 3
MODELS_G = 16
TILES_DEV = 32
STILES_DEV = 16
REQ = 16
CAP = 8
GCOLS = 384
TARGET_TILES = 1024
CELLS = 131072
SRC_TILES = 512
N_LAT = 4
N_LON = 8


def draw_requests(key, part):
    device_total = N_LAT * N_LON
    keys_all = jax.random.split(key, 4)
    heavy = jax.random.randint(keys_all[0], (GRIDS, device_total), 0, 3)
    offsets = jax.random.randint(keys_all[1], (GRIDS, device_total, 3), 0, STILES_DEV)
    perm_keys = jax.random.split(keys_all[2], GRIDS * device_total)
    others = jax.vmap(lambda single: jax.random.permutation(single, 2 * CAP)[:REQ - CAP])(perm_keys)
    others = others.reshape(GRIDS, device_total, REQ - CAP)
    order_keys = jax.random.split(keys_all[3], GRIDS * device_total)
    orders = jax.vmap(lambda single: jax.random.permutation(single, REQ))(order_keys).reshape(GRIDS, device_total, REQ)
    first_rel = jnp.broadcast_to(heavy[:, :, None], (GRIDS, device_total, CAP))
    first_rank = jnp.broadcast_to(jnp.arange(CAP, dtype=jnp.int32)[None, None, :], (GRIDS, device_total, CAP))
    other_index = others // CAP
    other_rel = other_index + (other_index >= heavy[:, :, None]).astype(jnp.int32)
    other_rank = others % CAP
    relative = jnp.concatenate([first_rel, other_rel], axis=2).astype(jnp.int32)
    ranking = jnp.concatenate([first_rank, other_rank], axis=2).astype(jnp.int32)
    chosen_offset = jnp.take_along_axis(offsets, relative, axis=2)
    local_tile = (chosen_offset + ranking) % STILES_DEV
    devices = jnp.arange(device_total, dtype=jnp.int32)[None, :, None]
    band = devices // N_LON
    sector = (devices % N_LON + relative - 1 + N_LON) % N_LON
    tiles = (band * N_LON + sector) * STILES_DEV + local_tile
    tiles = jnp.take_along_axis(tiles, orders, axis=2)
    return tiles.astype(jnp.int32)


def with_ends(drawn, key, smallest, top_value):
    longest = drawn.shape.index(max(drawn.shape))
    spots = []
    for shift in (0, 1):
        where = [jax.random.randint(jax.random.fold_in(key, axis), (), 0, length) for axis, length in enumerate(drawn.shape)]
        where[longest] = (where[longest] + shift) % drawn.shape[longest]
        spots.append(tuple(where))
    return drawn.at[spots[0]].set(smallest).at[spots[1]].set(top_value)


def levels(key, extent, cuts, low, top_value):
    factor_of = 1.0
    for position, shards_of in cuts:
        draws = jax.random.uniform(jax.random.fold_in(jax.random.fold_in(key, 6), position), (shards_of,), jnp.float32, low / len(cuts), top_value / len(cuts))
        factor_of = factor_of * jnp.repeat(jnp.exp(draws), extent[position] // shards_of).reshape((-1,) + (1,) * (len(extent) - 1 - position))
    return factor_of


def normal_values(own_key, shape, scale, most, cuts=(), kind=jnp.bfloat16):
    result = jax.random.normal(own_key, shape, jnp.float32) * scale
    if len(cuts) > 0:
        result = levels(own_key, shape, cuts, -0.22, 0.18) * result
    return jnp.clip(result, min=-most, max=most).astype(kind)


def setup_inputs(seed: int = 0) -> dict:
    keys = jax.random.split(jax.random.key(seed), 7)
    return {
        "fields": normal_values(keys[0], (GRIDS, SRC_TILES, TS, GCOLS), 1.0, 6.0, ((1, 32),)),
        "weights": normal_values(keys[1], (GRIDS, TARGET_TILES, MAXP, TS, TT), (TS * MAXP // 2) ** -0.5, 0.5, ((1, 32),)),
        "pair_slots": with_ends(jax.random.randint(keys[2], (GRIDS, TARGET_TILES, MAXP), 0, REQ), jax.random.fold_in(keys[2], 1), 0, REQ - 1).astype(jnp.int32),
        "pair_counts": with_ends(jax.random.randint(keys[3], (GRIDS, TARGET_TILES), 1, MAXP + 1), jax.random.fold_in(keys[3], 1), 1, MAXP).astype(jnp.int32),
        "requests": draw_requests(jax.random.fold_in(keys[6], 71), 0),
        "eofs": normal_values(keys[5], (EOFS, CELLS), CELLS ** -0.5, 0.015625, ((1, 32),)),
    }


def reference(fields, weights, pair_slots, pair_counts, requests, eofs):
    device_total = N_LAT * N_LON

    def one_device(running, device):
        start = device * TILES_DEV
        tile_weights = lax.dynamic_slice_in_dim(weights, start, TILES_DEV, 1)
        tile_slots = lax.dynamic_slice_in_dim(pair_slots, start, TILES_DEV, 1)
        tile_counts = lax.dynamic_slice_in_dim(pair_counts, start, TILES_DEV, 1)
        basis = lax.dynamic_slice_in_dim(eofs, start * TT, TILES_DEV * TT, 1)
        wanted = lax.dynamic_index_in_dim(requests, device, 1, keepdims=False)
        pieces = []
        for grid_id in range(GRIDS):
            tile_ids = wanted[grid_id][tile_slots[grid_id]]
            blocks = fields[grid_id][tile_ids]
            live_slots = jnp.arange(MAXP, dtype=jnp.int32)[None, :] < tile_counts[grid_id][:, None]
            masked = jnp.where(live_slots[:, :, None, None], tile_weights[grid_id], jnp.zeros((), jnp.bfloat16))
            regridded = jnp.einsum('tpsx,tpsc->txc', masked.astype(jnp.float32), blocks.astype(jnp.float32))
            by_model = regridded.reshape(TILES_DEV, TT, MODELS_G, MONTHS)
            anomaly = (by_model - jnp.mean(by_model, axis=3, keepdims=True)).astype(jnp.bfloat16)
            anomaly = anomaly.reshape(TILES_DEV * TT, MODELS_G * MONTHS)
            pieces.append(jnp.dot(basis, anomaly, preferred_element_type=jnp.float32))
        return running + jnp.concatenate(pieces, axis=1), None

    initial = jnp.zeros((EOFS, GRIDS * MODELS_G * MONTHS), jnp.float32)
    total, unused = lax.scan(one_device, initial, jnp.arange(device_total, dtype=jnp.int32))
    return total
```

```python
import functools

import jax
import jax.numpy as jnp
from jax import lax
from jax.experimental import pallas as pl
from jax.experimental.pallas import tpu as pltpu
from jax.sharding import PartitionSpec as P

TT = 128
MONTHS = 24
LANES = 128
MESH = pl.DeviceIdType.MESH


def split_terms(value):
    high = value.astype(jnp.bfloat16)
    rest = value - high.astype(jnp.float32)
    middle = rest.astype(jnp.bfloat16)
    low = (rest - middle.astype(jnp.float32)).astype(jnp.bfloat16)
    return high, middle, low


def basis_kernel(block, tiles, slot_ref, weight_ref, eof_ref, out_ref, *totals):
    step = pl.program_id(0)
    grids, _, pairs, cells, _ = weight_ref.shape
    modes = eof_ref.shape[0]

    @pl.when(step == 0)
    def _():
        for total in totals:
            total[...] = jnp.zeros_like(total)

    for t in range(block):
        rows = weight_ref[:, t].reshape(grids * pairs * cells, TT)
        basis = eof_ref[:, t * TT:(t + 1) * TT]
        product = lax.dot_general(
            rows, basis, (((1,), (1,)), ((), ())), preferred_element_type=jnp.float32
        )
        for p in range(pairs):
            for g in range(grids):
                slot = slot_ref[(g * tiles + step * block + t) * pairs + p]
                where = pl.ds(pl.multiple_of(slot * cells, cells), cells)
                start = (g * pairs + p) * cells
                totals[g][where, :modes] += product[start:start + cells]

    @pl.when(step == pl.num_programs(0) - 1)
    def _():
        height, width = out_ref.shape[1], totals[0].shape[1]
        for g in range(grids):
            for i, term in enumerate(split_terms(totals[g][:height])):
                out_ref[g, :, i * width:(i + 1) * width] = term


def project_kernel(rel_ref, tile_ref, before_ref, own_ref, after_ref, basis_ref, out_ref, source):
    grids, _, cells, columns = own_ref.shape
    _, chips, bands, rows, _ = out_ref.shape
    wanted = rel_ref.shape[0] // grids
    width = basis_ref.shape[2] // 3
    for g in range(grids):
        for j in range(wanted):
            rel, tile = rel_ref[g * wanted + j], tile_ref[g * wanted + j]
            side = jnp.where(rel == 0, before_ref[g, tile], after_ref[g, tile])
            source[j * cells:(j + 1) * cells] = jnp.where(rel == 1, own_ref[g, tile], side)
        product = lax.dot_general(
            source[...], basis_ref[g], (((0,), (0,)), ((), ())),
            preferred_element_type=jnp.float32,
        )
        total = product[:, 2 * width:] + product[:, width:2 * width] + product[:, :width]
        months = total.reshape(columns // MONTHS, MONTHS, width)
        months = months - jnp.mean(months, axis=1, keepdims=True)
        total = months.reshape(columns, width)
        first = g * columns
        for chunk in range(chips * bands):
            low = max(chunk * rows, first)
            high = min((chunk + 1) * rows, first + columns)
            for half in range(out_ref.shape[0]):
                if low < high:
                    out_ref[
                        half, chunk % chips, chunk // chips,
                        low - chunk * rows:high - chunk * rows, :,
                    ] = total[low - first:high - first, half * LANES:(half + 1) * LANES]


def reduce_kernel(
    part_ref, out_ref, core_in, plane_sum, plane_in, band_sum, band_in, final, other,
    core_send, core_recv, plane_send, plane_recv, band_send, band_recv, last_send, last_recv,
):
    _, chips, bands, _, _ = part_ref.shape
    lat, lon = lax.axis_index("lat"), lax.axis_index("lon")
    core, chip = lax.rem(lon, 2), lon // 2
    mate = (lat, chip * 2 + 1 - core)
    plane = [(lat, lax.rem(chip + i, chips) * 2 + core) for i in range(1, chips)]
    column = [(lax.rem(lat + j, bands), lon) for j in range(1, bands)]
    barrier = pltpu.get_barrier_semaphore()
    partners = [mate] + plane + column
    for partner in partners:
        pl.semaphore_signal(barrier, inc=1, device_id=partner, device_id_type=MESH)
    pl.semaphore_wait(barrier, len(partners))

    order = list(range(1, chips)) + [0]
    band_order = list(range(1, bands)) + [0]

    def send(source, target, send_sem, recv_sem, device):
        copy = pltpu.make_async_remote_copy(
            src_ref=source, dst_ref=target, send_sem=send_sem, recv_sem=recv_sem,
            device_id=device, device_id_type=MESH,
        )
        copy.start()
        return copy

    core_copies = {}
    for i in order:
        there = lax.rem(chip + i, chips)
        core_copies[i] = send(
            part_ref.at[1 - core, there], core_in.at[i], core_send.at[i], core_recv.at[i], mate
        )
    plane_copies = {}
    for i in order:
        there = lax.rem(chip + i, chips)
        core_copies[i].wait_recv()
        plane_sum[i] = part_ref[core, there] + core_in[i]
        if i > 0:
            for j in band_order:
                band = lax.rem(lat + j, bands)
                plane_copies[i, j] = send(
                    plane_sum.at[i, band], plane_in.at[i - 1, j],
                    plane_send.at[i - 1, j], plane_recv.at[i - 1, j], plane[i - 1],
                )
    band_copies = {}
    for j in band_order:
        band = lax.rem(lat + j, bands)
        total = plane_sum[0, band]
        for i in range(1, chips):
            plane_copies[i, j].wait_recv()
            total = total + plane_in[i - 1, j]
        band_sum[j] = total
        if j > 0:
            band_copies[j] = send(
                band_sum.at[j], band_in.at[j - 1], band_send.at[j - 1], band_recv.at[j - 1],
                column[j - 1],
            )
    total = band_sum[0]
    for j in range(1, bands):
        band_copies[j].wait_recv()
        total = total + band_in[j - 1]
    final[...] = total
    last = send(final, other, last_send, last_recv, mate)
    out_ref[core] = total
    last.wait_recv()
    out_ref[1 - core] = other[...]
    for copy in [*core_copies.values(), *plane_copies.values(), *band_copies.values(), last]:
        copy.wait_send()


def shards(fields, weights, pair_slots, pair_counts, requests, eofs):
    lat_count, lon_count = lax.axis_size("lat"), lax.axis_size("lon")
    lat_index, lon_index = lax.axis_index("lat"), lax.axis_index("lon")
    device = lat_index * lon_count + lon_index
    grids, src_tiles, cells, columns = fields.shape
    tiles, pairs = weights.shape[1], weights.shape[2]
    modes = eofs.shape[0]
    asked = requests.shape[2]
    up = [(i, (i + 1) % lon_count) for i in range(lon_count)]
    down = [(j, i) for i, j in up]
    before = lax.ppermute(fields, "lon", up)
    after = lax.ppermute(fields, "lon", down)

    wanted = lax.dynamic_index_in_dim(requests, device, 1, keepdims=False).reshape(-1)
    sector = wanted // src_tiles - lat_index * lon_count
    relative = (sector - lon_index + 1 + lon_count) % lon_count
    local_tiles = wanted % src_tiles
    live = jnp.arange(pairs, dtype=jnp.int32) < pair_counts[:, :, None]
    slots = jnp.where(live, pair_slots, asked).reshape(-1)

    halves = 2
    width = halves * LANES
    block = 4
    while tiles % block:
        block //= 2
    basis = pl.pallas_call(
        functools.partial(basis_kernel, block, tiles),
        out_shape=jax.ShapeDtypeStruct((grids, asked * cells, 3 * width), jnp.bfloat16),
        grid_spec=pltpu.PrefetchScalarGridSpec(
            num_scalar_prefetch=1,
            grid=(tiles // block,),
            in_specs=[
                pl.BlockSpec((grids, block, pairs, cells, TT), lambda s, _: (0, s, 0, 0, 0)),
                pl.BlockSpec((modes, block * TT), lambda s, _: (0, s)),
            ],
            out_specs=pl.BlockSpec((grids, asked * cells, 3 * width), lambda s, _: (0, 0, 0)),
            scratch_shapes=[pltpu.VMEM(((asked + 1) * cells, width), jnp.float32)] * grids,
        ),
        cost_estimate=pl.CostEstimate(
            flops=2 * weights.size * modes, bytes_accessed=2 * (weights.size + eofs.size),
            transcendentals=0,
        ),
    )(slots, weights, eofs)

    chips = lon_count // 2
    rows = grids * columns // (lat_count * chips)
    smem = pl.BlockSpec(memory_space=pltpu.SMEM)
    vmem = pl.BlockSpec(memory_space=pltpu.VMEM)
    part = pl.pallas_call(
        project_kernel,
        out_shape=jax.ShapeDtypeStruct((halves, chips, lat_count, rows, LANES), jnp.float32),
        in_specs=[smem, smem, vmem, vmem, vmem, vmem],
        out_specs=vmem,
        scratch_shapes=[pltpu.VMEM((asked * cells, columns), jnp.bfloat16)],
    )(relative, local_tiles, before, fields, after, basis)

    dma = pltpu.SemaphoreType.DMA
    buffer = lambda *shape: pltpu.VMEM((*shape, rows, LANES), jnp.float32)
    summed = pl.pallas_call(
        reduce_kernel,
        out_shape=jax.ShapeDtypeStruct((halves, rows, LANES), jnp.float32),
        in_specs=[vmem],
        out_specs=vmem,
        scratch_shapes=[
            buffer(chips, lat_count), buffer(chips, lat_count), buffer(chips - 1, lat_count),
            buffer(lat_count), buffer(lat_count - 1), buffer(), buffer(),
            dma((chips,)), dma((chips,)),
            dma((chips - 1, lat_count)), dma((chips - 1, lat_count)),
            dma((lat_count - 1,)), dma((lat_count - 1,)),
            dma(()), dma(()),
        ],
        compiler_params=pltpu.CompilerParams(collective_id=0, has_side_effects=True),
    )(part)
    mine = lax.dynamic_slice_in_dim(summed, lax.rem(lon_index, 2) * (rows // 2), rows // 2, 1)
    joined = jnp.transpose(mine, (0, 2, 1)).reshape(width, rows // 2)
    return joined[:modes]


def solution(mesh):
    return jax.shard_map(
        shards,
        mesh=mesh,
        in_specs=(
            P(None, ("lat", "lon"), None, None),
            P(None, ("lat", "lon"), None, None, None),
            P(None, ("lat", "lon"), None),
            P(None, ("lat", "lon")),
            P(),
            P(None, ("lat", "lon")),
        ),
        out_specs=P(None, ("lat", "lon")),
        check_vma=False,
    )
```

```python
import functools

import jax
import jax.numpy as jnp
from jax import lax
from jax.experimental import pallas as pl
from jax.experimental.pallas import tpu as pltpu
from jax.sharding import PartitionSpec as P

TT = 128
MONTHS = 24
LANES = 128
MESH = pl.DeviceIdType.MESH


def split_terms(value):
    high = value.astype(jnp.bfloat16)
    rest = value - high.astype(jnp.float32)
    middle = rest.astype(jnp.bfloat16)
    low = (rest - middle.astype(jnp.float32)).astype(jnp.bfloat16)
    return high, middle, low


def basis_kernel(block, tiles, slot_ref, weight_ref, eof_ref, out_ref, *totals):
    step = pl.program_id(0)
    grids, _, pairs, cells, _ = weight_ref.shape
    modes = eof_ref.shape[0]

    @pl.when(step == 0)
    def _():
        for total in totals:
            total[...] = jnp.zeros_like(total)

    for t in range(block):
        rows = weight_ref[:, t].reshape(grids * pairs * cells, TT)
        basis = eof_ref[:, t * TT:(t + 1) * TT]
        product = lax.dot_general(
            rows, basis, (((1,), (1,)), ((), ())), preferred_element_type=jnp.float32
        )
        for p in range(pairs):
            for g in range(grids):
                slot = slot_ref[(g * tiles + step * block + t) * pairs + p]
                where = pl.ds(pl.multiple_of(slot * cells, cells), cells)
                start = (g * pairs + p) * cells
                totals[g][where, :modes] += product[start:start + cells]

    @pl.when(step == pl.num_programs(0) - 1)
    def _():
        height, width = out_ref.shape[1], totals[0].shape[1]
        for g in range(grids):
            for i, term in enumerate(split_terms(totals[g][:height])):
                out_ref[g, :, i * width:(i + 1) * width] = term


def pack_kernel(request_ref, own_ref, up_ref, down_ref):
    grids, src_tiles, _, _ = own_ref.shape
    lon_count = lax.axis_size("lon")
    lat, lon = lax.axis_index("lat"), lax.axis_index("lon")
    first = (lat * lon_count + lon) * src_tiles
    for target, shift in ((up_ref, 1), (down_ref, lon_count - 1)):
        asker = lat * lon_count + lax.rem(lon + shift, lon_count)
        for g in range(grids):
            def place(q, count, g=g, target=target, asker=asker):
                tile = request_ref[g, q, asker] - first
                held = jnp.logical_and(tile >= 0, tile < src_tiles)

                @pl.when(held)
                def _():
                    target[g, count] = own_ref[g, tile]

                return count + held.astype(jnp.int32)

            lax.fori_loop(0, request_ref.shape[1], place, jnp.int32(0), unroll=True)


def project(rel_ref, near_ref, tile_ref, before_ref, own_ref, after_ref, basis_ref, part, source):
    grids, _, cells, columns = own_ref.shape
    _, chips, bands, rows, _ = part.shape
    wanted = rel_ref.shape[0] // grids
    width = basis_ref.shape[2] // 3
    for g in range(grids):
        for j in range(wanted):
            k = g * wanted + j
            rel, near, tile = rel_ref[k], near_ref[k], tile_ref[k]
            side = jnp.where(rel == 0, before_ref[g, near], after_ref[g, near])
            source[j * cells:(j + 1) * cells] = jnp.where(rel == 1, own_ref[g, tile], side)
        product = lax.dot_general(
            source[...], basis_ref[g], (((0,), (0,)), ((), ())),
            preferred_element_type=jnp.float32,
        )
        total = product[:, 2 * width:] + product[:, width:2 * width] + product[:, :width]
        months = total.reshape(columns // MONTHS, MONTHS, width)
        months = months - jnp.mean(months, axis=1, keepdims=True)
        total = months.reshape(columns, width)
        first = g * columns
        for chunk in range(chips * bands):
            low = max(chunk * rows, first)
            high = min((chunk + 1) * rows, first + columns)
            for half in range(part.shape[0]):
                if low < high:
                    part[
                        half, chunk % chips, chunk // chips,
                        low - chunk * rows:high - chunk * rows, :,
                    ] = total[low - first:high - first, half * LANES:(half + 1) * LANES]


def reduce_kernel(
    rel_ref, near_ref, tile_ref, before_ref, own_ref, after_ref, basis_ref, out_ref,
    source, part, core_in, plane_sum, plane_in, band_sum, band_in, final, other,
    core_send, core_recv, plane_send, plane_recv, band_send, band_recv, last_send, last_recv,
):
    _, chips, bands, _, _ = part.shape
    lat, lon = lax.axis_index("lat"), lax.axis_index("lon")
    core, chip = lax.rem(lon, 2), lon // 2
    mate = (lat, chip * 2 + 1 - core)
    plane = [(lat, lax.rem(chip + i, chips) * 2 + core) for i in range(1, chips)]
    column = [(lax.rem(lat + j, bands), lon) for j in range(1, bands)]
    barrier = pltpu.get_barrier_semaphore()
    partners = [mate] + plane + column
    for partner in partners:
        pl.semaphore_signal(barrier, inc=1, device_id=partner, device_id_type=MESH)
    project(
        rel_ref, near_ref, tile_ref, before_ref, own_ref, after_ref, basis_ref, part, source
    )
    pl.semaphore_wait(barrier, len(partners))

    order = list(range(1, chips)) + [0]
    band_order = list(range(1, bands)) + [0]

    def send(source, target, send_sem, recv_sem, device):
        copy = pltpu.make_async_remote_copy(
            src_ref=source, dst_ref=target, send_sem=send_sem, recv_sem=recv_sem,
            device_id=device, device_id_type=MESH,
        )
        copy.start()
        return copy

    copies, arrivals = [], {}
    for j in band_order:
        for i in order:
            there, band = lax.rem(chip + i, chips), lax.rem(lat + j, bands)
            arrivals["core", i, j] = send(
                part.at[1 - core, there, band], core_in.at[i, j],
                core_send.at[i, j], core_recv.at[i, j], mate,
            )
    for j in band_order:
        for i in order:
            there, band = lax.rem(chip + i, chips), lax.rem(lat + j, bands)
            arrivals["core", i, j].wait_recv()
            plane_sum[i, j] = part[core, there, band] + core_in[i, j]
            if i > 0:
                arrivals["plane", i, j] = send(
                    plane_sum.at[i, j], plane_in.at[i - 1, j],
                    plane_send.at[i - 1, j], plane_recv.at[i - 1, j], plane[i - 1],
                )
    for j in band_order:
        total = plane_sum[0, j]
        for i in range(1, chips):
            arrivals["plane", i, j].wait_recv()
            total = total + plane_in[i - 1, j]
        band_sum[j] = total
        if j > 0:
            arrivals["band", j] = send(
                band_sum.at[j], band_in.at[j - 1], band_send.at[j - 1], band_recv.at[j - 1],
                column[j - 1],
            )
    total = band_sum[0]
    for j in range(1, bands):
        arrivals["band", j].wait_recv()
        total = total + band_in[j - 1]
    final[...] = total
    arrivals["last"] = send(final, other, last_send, last_recv, mate)
    arrivals["last"].wait_recv()
    theirs = other[...]
    left = jnp.where(core == 0, total, theirs)
    right = jnp.where(core == 0, theirs, total)
    joined = jnp.concatenate([left, right], axis=1)
    height, modes = out_ref.shape
    out_ref[...] = jnp.where(core == 0, joined[:height], joined[height:])[:, :modes]
    for copy in arrivals.values():
        copy.wait_send()


def shards(fields, weights, pair_slots, pair_counts, requests, eofs):
    lat_count, lon_count = lax.axis_size("lat"), lax.axis_size("lon")
    lat_index, lon_index = lax.axis_index("lat"), lax.axis_index("lon")
    device = lat_index * lon_count + lon_index
    grids, src_tiles, cells, columns = fields.shape
    tiles, pairs = weights.shape[1], weights.shape[2]
    modes = eofs.shape[0]
    asked = requests.shape[2]
    up = [(i, (i + 1) % lon_count) for i in range(lon_count)]
    down = [(j, i) for i, j in up]
    smem = pl.BlockSpec(memory_space=pltpu.SMEM)
    vmem = pl.BlockSpec(memory_space=pltpu.VMEM)
    packed = jax.ShapeDtypeStruct((grids, asked // 2, cells, columns), fields.dtype)
    upward, downward = pl.pallas_call(
        pack_kernel, out_shape=[packed, packed], in_specs=[smem, vmem], out_specs=[vmem, vmem],
    )(jnp.transpose(requests, (0, 2, 1)), fields)
    before = lax.ppermute(upward, "lon", up)
    after = lax.ppermute(downward, "lon", down)

    wanted = lax.dynamic_index_in_dim(requests, device, 1, keepdims=False)
    sector = wanted // src_tiles - lat_index * lon_count
    relative = (sector - lon_index + 1 + lon_count) % lon_count
    earlier = jnp.arange(asked)[None, :] < jnp.arange(asked)[:, None]
    same = (relative[:, :, None] == relative[:, None, :]) & earlier
    rank = jnp.sum(same, axis=2, dtype=jnp.int32)
    near = jnp.where(relative == 1, 0, rank).reshape(-1)
    local_tiles = jnp.where(relative == 1, wanted % src_tiles, 0).reshape(-1)
    relative = relative.reshape(-1)
    live = jnp.arange(pairs, dtype=jnp.int32) < pair_counts[:, :, None]
    slots = jnp.where(live, pair_slots, asked).reshape(-1)

    halves = 2
    width = halves * LANES
    block = 4
    while tiles % block:
        block //= 2
    basis = pl.pallas_call(
        functools.partial(basis_kernel, block, tiles),
        out_shape=jax.ShapeDtypeStruct((grids, asked * cells, 3 * width), jnp.bfloat16),
        grid_spec=pltpu.PrefetchScalarGridSpec(
            num_scalar_prefetch=1,
            grid=(tiles // block,),
            in_specs=[
                pl.BlockSpec((grids, block, pairs, cells, TT), lambda s, _: (0, s, 0, 0, 0)),
                pl.BlockSpec((modes, block * TT), lambda s, _: (0, s)),
            ],
            out_specs=pl.BlockSpec((grids, asked * cells, 3 * width), lambda s, _: (0, 0, 0)),
            scratch_shapes=[pltpu.VMEM(((asked + 1) * cells, width), jnp.float32)] * grids,
        ),
        cost_estimate=pl.CostEstimate(
            flops=2 * weights.size * modes, bytes_accessed=2 * (weights.size + eofs.size),
            transcendentals=0,
        ),
    )(slots, weights, eofs)

    chips = lon_count // 2
    rows = grids * columns // (lat_count * chips)
    dma = pltpu.SemaphoreType.DMA
    buffer = lambda *shape: pltpu.VMEM((*shape, rows, LANES), jnp.float32)
    summed = pl.pallas_call(
        reduce_kernel,
        out_shape=jax.ShapeDtypeStruct((rows // 2, modes), jnp.float32),
        in_specs=[smem, smem, smem, vmem, vmem, vmem, vmem],
        out_specs=vmem,
        scratch_shapes=[
            pltpu.VMEM((asked * cells, columns), jnp.bfloat16),
            buffer(halves, chips, lat_count),
            buffer(chips, lat_count), buffer(chips, lat_count), buffer(chips - 1, lat_count),
            buffer(lat_count), buffer(lat_count - 1), buffer(), buffer(),
            dma((chips, lat_count)), dma((chips, lat_count)),
            dma((chips - 1, lat_count)), dma((chips - 1, lat_count)),
            dma((lat_count - 1,)), dma((lat_count - 1,)),
            dma(()), dma(()),
        ],
        compiler_params=pltpu.CompilerParams(collective_id=0, has_side_effects=True),
    )(relative, near, local_tiles, before, fields, after, basis)
    return jnp.transpose(summed)


def solution(mesh):
    return jax.shard_map(
        shards,
        mesh=mesh,
        in_specs=(
            P(None, ("lat", "lon"), None, None),
            P(None, ("lat", "lon"), None, None, None),
            P(None, ("lat", "lon"), None),
            P(None, ("lat", "lon")),
            P(),
            P(None, ("lat", "lon")),
        ),
        out_specs=P(None, ("lat", "lon")),
        check_vma=False,
    )
```

```python
import functools

import jax
import jax.numpy as jnp
from jax import lax
from jax.experimental import pallas as pl
from jax.experimental.pallas import tpu as pltpu
from jax.sharding import PartitionSpec as P

TT = 128
MONTHS = 24
LANES = 128
MESH = pl.DeviceIdType.MESH
VMEM_LIMIT = 20 << 20


def split_terms(value):
    high = value.astype(jnp.bfloat16)
    rest = value - high.astype(jnp.float32)
    middle = rest.astype(jnp.bfloat16)
    low = (rest - middle.astype(jnp.float32)).astype(jnp.bfloat16)
    return high, middle, low


def basis_kernel(block, tiles, slot_ref, weight_ref, eof_ref, out_ref, *totals):
    step = pl.program_id(0)
    grids, _, pairs, cells, _ = weight_ref.shape
    modes = eof_ref.shape[0]

    @pl.when(step == 0)
    def _():
        for total in totals:
            total[...] = jnp.zeros_like(total)

    for t in range(block):
        rows = weight_ref[:, t].reshape(grids * pairs * cells, TT)
        basis = eof_ref[:, t * TT:(t + 1) * TT]
        product = lax.dot_general(
            rows, basis, (((1,), (1,)), ((), ())), preferred_element_type=jnp.float32
        )
        for p in range(pairs):
            for g in range(grids):
                slot = slot_ref[(g * tiles + step * block + t) * pairs + p]
                where = pl.ds(pl.multiple_of(slot * cells, cells), cells)
                start = (g * pairs + p) * cells
                totals[g][where, :modes] += product[start:start + cells]

    @pl.when(step == pl.num_programs(0) - 1)
    def _():
        height, width = out_ref.shape[1], totals[0].shape[1]
        for g in range(grids):
            for i, term in enumerate(split_terms(totals[g][:height])):
                out_ref[g, :, i * width:(i + 1) * width] = term


def pack_kernel(request_ref, own_ref, up_ref, down_ref):
    grids, src_tiles, _, _ = own_ref.shape
    lon_count = lax.axis_size("lon")
    lat, lon = lax.axis_index("lat"), lax.axis_index("lon")
    first = (lat * lon_count + lon) * src_tiles
    for target, shift in ((up_ref, 1), (down_ref, lon_count - 1)):
        asker = lat * lon_count + lax.rem(lon + shift, lon_count)
        for g in range(grids):
            def place(q, count, g=g, target=target, asker=asker):
                tile = request_ref[g, q, asker] - first
                held = jnp.logical_and(tile >= 0, tile < src_tiles)

                @pl.when(held)
                def _():
                    target[g, count] = own_ref[g, tile]

                return count + held.astype(jnp.int32)

            lax.fori_loop(0, request_ref.shape[1], place, jnp.int32(0), unroll=True)


def project(rel_ref, near_ref, tile_ref, before_ref, own_ref, after_ref, basis_ref, part, source):
    grids, _, cells, columns = own_ref.shape
    _, chips, bands, rows, _ = part.shape
    wanted = rel_ref.shape[0] // grids
    width = basis_ref.shape[2] // 3
    for g in range(grids):
        for j in range(wanted):
            k = g * wanted + j
            rel, near, tile = rel_ref[k], near_ref[k], tile_ref[k]
            side = jnp.where(rel == 0, before_ref[g, near], after_ref[g, near])
            source[j * cells:(j + 1) * cells] = jnp.where(rel == 1, own_ref[g, tile], side)
        product = lax.dot_general(
            source[...], basis_ref[g], (((0,), (0,)), ((), ())),
            preferred_element_type=jnp.float32,
        )
        total = product[:, 2 * width:] + product[:, width:2 * width] + product[:, :width]
        months = total.reshape(columns // MONTHS, MONTHS, width)
        months = months - jnp.mean(months, axis=1, keepdims=True)
        total = months.reshape(columns, width)
        first = g * columns
        for chunk in range(chips * bands):
            low = max(chunk * rows, first)
            high = min((chunk + 1) * rows, first + columns)
            for half in range(part.shape[0]):
                if low < high:
                    part[
                        half, chunk % chips, chunk // chips,
                        low - chunk * rows:high - chunk * rows, :,
                    ] = total[low - first:high - first, half * LANES:(half + 1) * LANES]


def reduce_kernel(
    rel_ref, near_ref, tile_ref, before_ref, own_ref, after_ref, basis_ref, out_ref,
    source, part, core_in, plane_sum, plane_in, band_sum, band_in, final, other,
    core_send, core_recv, plane_send, plane_recv, band_send, band_recv, last_send, last_recv,
):
    _, chips, bands, _, _ = part.shape
    lat, lon = lax.axis_index("lat"), lax.axis_index("lon")
    core, chip = lax.rem(lon, 2), lon // 2
    mate = (lat, chip * 2 + 1 - core)
    plane = [(lat, lax.rem(chip + i, chips) * 2 + core) for i in range(1, chips)]
    column = [(lax.rem(lat + j, bands), lon) for j in range(1, bands)]
    barrier = pltpu.get_barrier_semaphore()
    partners = [mate] + plane + column
    for partner in partners:
        pl.semaphore_signal(barrier, inc=1, device_id=partner, device_id_type=MESH)
    project(
        rel_ref, near_ref, tile_ref, before_ref, own_ref, after_ref, basis_ref, part, source
    )
    pl.semaphore_wait(barrier, len(partners))

    order = list(range(1, chips)) + [0]
    band_order = list(range(1, bands)) + [0]

    def send(source, target, send_sem, recv_sem, device):
        copy = pltpu.make_async_remote_copy(
            src_ref=source, dst_ref=target, send_sem=send_sem, recv_sem=recv_sem,
            device_id=device, device_id_type=MESH,
        )
        copy.start()
        return copy

    copies, arrivals = [], {}
    for j in band_order:
        for i in order:
            there, band = lax.rem(chip + i, chips), lax.rem(lat + j, bands)
            arrivals["core", i, j] = send(
                part.at[1 - core, there, band], core_in.at[i, j],
                core_send.at[i, j], core_recv.at[i, j], mate,
            )
    for j in band_order:
        for i in order:
            there, band = lax.rem(chip + i, chips), lax.rem(lat + j, bands)
            arrivals["core", i, j].wait_recv()
            plane_sum[i, j] = part[core, there, band] + core_in[i, j]
            if i > 0:
                arrivals["plane", i, j] = send(
                    plane_sum.at[i, j], plane_in.at[i - 1, j],
                    plane_send.at[i - 1, j], plane_recv.at[i - 1, j], plane[i - 1],
                )
    for j in band_order:
        total = plane_sum[0, j]
        for i in range(1, chips):
            arrivals["plane", i, j].wait_recv()
            total = total + plane_in[i - 1, j]
        band_sum[j] = total
        if j > 0:
            arrivals["band", j] = send(
                band_sum.at[j], band_in.at[j - 1], band_send.at[j - 1], band_recv.at[j - 1],
                column[j - 1],
            )
    total = band_sum[0]
    for j in range(1, bands):
        arrivals["band", j].wait_recv()
        total = total + band_in[j - 1]
    final[...] = total
    arrivals["last"] = send(final, other, last_send, last_recv, mate)
    arrivals["last"].wait_recv()
    theirs = other[...]
    left = jnp.where(core == 0, total, theirs)
    right = jnp.where(core == 0, theirs, total)
    joined = jnp.concatenate([left, right], axis=1)
    height, modes = out_ref.shape
    out_ref[...] = jnp.where(core == 0, joined[:height], joined[height:])[:, :modes]
    for copy in arrivals.values():
        copy.wait_send()


def shards(fields, weights, pair_slots, pair_counts, requests, eofs):
    lat_count, lon_count = lax.axis_size("lat"), lax.axis_size("lon")
    lat_index, lon_index = lax.axis_index("lat"), lax.axis_index("lon")
    device = lat_index * lon_count + lon_index
    grids, src_tiles, cells, columns = fields.shape
    tiles, pairs = weights.shape[1], weights.shape[2]
    modes = eofs.shape[0]
    asked = requests.shape[2]
    up = [(i, (i + 1) % lon_count) for i in range(lon_count)]
    down = [(j, i) for i, j in up]
    smem = pl.BlockSpec(memory_space=pltpu.SMEM)
    vmem = pl.BlockSpec(memory_space=pltpu.VMEM)
    packed = jax.ShapeDtypeStruct((grids, asked // 2, cells, columns), fields.dtype)
    upward, downward = pl.pallas_call(
        pack_kernel, out_shape=[packed, packed], in_specs=[smem, vmem], out_specs=[vmem, vmem],
        compiler_params=pltpu.CompilerParams(vmem_limit_bytes=VMEM_LIMIT),
    )(jnp.transpose(requests, (0, 2, 1)), fields)
    before = lax.ppermute(upward, "lon", up)
    after = lax.ppermute(downward, "lon", down)

    wanted = lax.dynamic_index_in_dim(requests, device, 1, keepdims=False)
    sector = wanted // src_tiles - lat_index * lon_count
    relative = (sector - lon_index + 1 + lon_count) % lon_count
    earlier = jnp.arange(asked)[None, :] < jnp.arange(asked)[:, None]
    same = (relative[:, :, None] == relative[:, None, :]) & earlier
    rank = jnp.sum(same, axis=2, dtype=jnp.int32)
    near = jnp.where(relative == 1, 0, rank).reshape(-1)
    local_tiles = jnp.where(relative == 1, wanted % src_tiles, 0).reshape(-1)
    relative = relative.reshape(-1)
    live = jnp.arange(pairs, dtype=jnp.int32) < pair_counts[:, :, None]
    slots = jnp.where(live, pair_slots, asked).reshape(-1)

    halves = 2
    width = halves * LANES
    block = 4
    while tiles % block:
        block //= 2
    basis = pl.pallas_call(
        functools.partial(basis_kernel, block, tiles),
        out_shape=jax.ShapeDtypeStruct((grids, asked * cells, 3 * width), jnp.bfloat16),
        grid_spec=pltpu.PrefetchScalarGridSpec(
            num_scalar_prefetch=1,
            grid=(tiles // block,),
            in_specs=[
                pl.BlockSpec((grids, block, pairs, cells, TT), lambda s, _: (0, s, 0, 0, 0)),
                pl.BlockSpec((modes, block * TT), lambda s, _: (0, s)),
            ],
            out_specs=pl.BlockSpec((grids, asked * cells, 3 * width), lambda s, _: (0, 0, 0)),
            scratch_shapes=[pltpu.VMEM(((asked + 1) * cells, width), jnp.float32)] * grids,
        ),
        compiler_params=pltpu.CompilerParams(vmem_limit_bytes=VMEM_LIMIT),
        cost_estimate=pl.CostEstimate(
            flops=2 * weights.size * modes, bytes_accessed=2 * (weights.size + eofs.size),
            transcendentals=0,
        ),
    )(slots, weights, eofs)

    chips = lon_count // 2
    rows = grids * columns // (lat_count * chips)
    dma = pltpu.SemaphoreType.DMA
    buffer = lambda *shape: pltpu.VMEM((*shape, rows, LANES), jnp.float32)
    summed = pl.pallas_call(
        reduce_kernel,
        out_shape=jax.ShapeDtypeStruct((rows // 2, modes), jnp.float32),
        in_specs=[smem, smem, smem, vmem, vmem, vmem, vmem],
        out_specs=vmem,
        scratch_shapes=[
            pltpu.VMEM((asked * cells, columns), jnp.bfloat16),
            buffer(halves, chips, lat_count),
            buffer(chips, lat_count), buffer(chips, lat_count), buffer(chips - 1, lat_count),
            buffer(lat_count), buffer(lat_count - 1), buffer(), buffer(),
            dma((chips, lat_count)), dma((chips, lat_count)),
            dma((chips - 1, lat_count)), dma((chips - 1, lat_count)),
            dma((lat_count - 1,)), dma((lat_count - 1,)),
            dma(()), dma(()),
        ],
        compiler_params=pltpu.CompilerParams(
            collective_id=0, has_side_effects=True, vmem_limit_bytes=VMEM_LIMIT
        ),
    )(relative, near, local_tiles, before, fields, after, basis)
    return jnp.transpose(summed)


def solution(mesh):
    return jax.shard_map(
        shards,
        mesh=mesh,
        in_specs=(
            P(None, ("lat", "lon"), None, None),
            P(None, ("lat", "lon"), None, None, None),
            P(None, ("lat", "lon"), None),
            P(None, ("lat", "lon")),
            P(),
            P(None, ("lat", "lon")),
        ),
        out_specs=P(None, ("lat", "lon")),
        check_vma=False,
    )
```

```python
import functools

import jax
import jax.numpy as jnp
from jax import lax
from jax.experimental import pallas as pl
from jax.experimental.pallas import tpu as pltpu
from jax.sharding import PartitionSpec as P

TT = 128
MONTHS = 24
LANES = 128
MESH = pl.DeviceIdType.MESH
VMEM_LIMIT = 20 << 20


def split_terms(value):
    high = value.astype(jnp.bfloat16)
    rest = value - high.astype(jnp.float32)
    middle = rest.astype(jnp.bfloat16)
    low = (rest - middle.astype(jnp.float32)).astype(jnp.bfloat16)
    return high, middle, low


def basis_kernel(block, tiles, slot_ref, weight_ref, eof_ref, out_ref, *totals):
    step = pl.program_id(0)
    grids, _, pairs, cells, _ = weight_ref.shape
    modes = eof_ref.shape[0]
    ways = len(totals) // grids

    @pl.when(step == 0)
    def _():
        for total in totals:
            total[...] = jnp.zeros_like(total)

    for t in range(block):
        rows = weight_ref[:, t].reshape(grids * pairs * cells, TT)
        basis = eof_ref[:, t * TT:(t + 1) * TT]
        product = lax.dot_general(
            rows, basis, (((1,), (1,)), ((), ())), preferred_element_type=jnp.float32
        )
        for p in range(pairs):
            for g in range(grids):
                slot = slot_ref[(g * tiles + step * block + t) * pairs + p]
                where = pl.ds(pl.multiple_of(slot * cells, cells), cells)
                start = (g * pairs + p) * cells
                totals[g * ways + p % ways][where, :modes] += product[start:start + cells]

    @pl.when(step == pl.num_programs(0) - 1)
    def _():
        height, width = out_ref.shape[1], totals[0].shape[1]
        for g in range(grids):
            total = totals[g * ways][:height]
            for way in range(1, ways):
                total = total + totals[g * ways + way][:height]
            for i, term in enumerate(split_terms(total)):
                out_ref[g, :, i * width:(i + 1) * width] = term


def pack_kernel(request_ref, own_ref, up_ref, down_ref):
    grids, src_tiles, _, _ = own_ref.shape
    lon_count = lax.axis_size("lon")
    lat, lon = lax.axis_index("lat"), lax.axis_index("lon")
    first = (lat * lon_count + lon) * src_tiles
    for target, shift in ((up_ref, 1), (down_ref, lon_count - 1)):
        asker = lat * lon_count + lax.rem(lon + shift, lon_count)
        for g in range(grids):
            def place(q, count, g=g, target=target, asker=asker):
                tile = request_ref[g, q, asker] - first
                held = jnp.logical_and(tile >= 0, tile < src_tiles)

                @pl.when(held)
                def _():
                    target[g, count] = own_ref[g, tile]

                return count + held.astype(jnp.int32)

            lax.fori_loop(0, request_ref.shape[1], place, jnp.int32(0), unroll=True)


def project(table_ref, before_ref, own_ref, after_ref, basis_ref, part, source):
    grids, _, cells, columns = own_ref.shape
    _, chips, bands, rows, _ = part.shape
    wanted = basis_ref.shape[1] // cells
    offset = table_ref.shape[0] - grids * wanted
    src_tiles = own_ref.shape[1]
    width = basis_ref.shape[2] // 3
    for g in range(grids):
        for j in range(wanted):
            code = table_ref[offset + g * wanted + j]
            rel, index = code // src_tiles, code % src_tiles
            near, tile = jnp.where(rel == 1, 0, index), jnp.where(rel == 1, index, 0)
            side = jnp.where(rel == 0, before_ref[g, near], after_ref[g, near])
            source[j * cells:(j + 1) * cells] = jnp.where(rel == 1, own_ref[g, tile], side)
        product = lax.dot_general(
            source[...], basis_ref[g], (((0,), (0,)), ((), ())),
            preferred_element_type=jnp.float32,
        )
        total = product[:, 2 * width:] + product[:, width:2 * width] + product[:, :width]
        months = total.reshape(columns // MONTHS, MONTHS, width)
        months = months - jnp.mean(months, axis=1, keepdims=True)
        total = months.reshape(columns, width)
        first = g * columns
        for chunk in range(chips * bands):
            low = max(chunk * rows, first)
            high = min((chunk + 1) * rows, first + columns)
            for half in range(part.shape[0]):
                if low < high:
                    part[
                        half, chunk % chips, chunk // chips,
                        low - chunk * rows:high - chunk * rows, :,
                    ] = total[low - first:high - first, half * LANES:(half + 1) * LANES]


def reduce_kernel(
    table_ref, before_ref, own_ref, after_ref, basis_ref, out_ref,
    source, part, core_in, plane_sum, plane_in, band_sum, band_in, final, other,
    core_send, core_recv, plane_send, plane_recv, band_send, band_recv, last_send, last_recv,
):
    _, chips, bands, _, _ = part.shape
    lat, lon = lax.axis_index("lat"), lax.axis_index("lon")
    core, chip = lax.rem(lon, 2), lon // 2
    mate = (lat, chip * 2 + 1 - core)
    plane = [(lat, lax.rem(chip + i, chips) * 2 + core) for i in range(1, chips)]
    column = [(lax.rem(lat + j, bands), lon) for j in range(1, bands)]
    barrier = pltpu.get_barrier_semaphore()
    partners = [mate] + plane + column
    for partner in partners:
        pl.semaphore_signal(barrier, inc=1, device_id=partner, device_id_type=MESH)
    project(table_ref, before_ref, own_ref, after_ref, basis_ref, part, source)
    pl.semaphore_wait(barrier, len(partners))

    order = list(range(1, chips)) + [0]
    band_order = list(range(1, bands)) + [0]

    def send(source, target, send_sem, recv_sem, device):
        copy = pltpu.make_async_remote_copy(
            src_ref=source, dst_ref=target, send_sem=send_sem, recv_sem=recv_sem,
            device_id=device, device_id_type=MESH,
        )
        copy.start()
        return copy

    copies, arrivals = [], {}
    for j in band_order:
        for i in order:
            there, band = lax.rem(chip + i, chips), lax.rem(lat + j, bands)
            arrivals["core", i, j] = send(
                part.at[1 - core, there, band], core_in.at[i, j],
                core_send.at[i, j], core_recv.at[i, j], mate,
            )
    for j in band_order:
        for i in order:
            there, band = lax.rem(chip + i, chips), lax.rem(lat + j, bands)
            arrivals["core", i, j].wait_recv()
            plane_sum[i, j] = part[core, there, band] + core_in[i, j]
            if i > 0:
                arrivals["plane", i, j] = send(
                    plane_sum.at[i, j], plane_in.at[i - 1, j],
                    plane_send.at[i - 1, j], plane_recv.at[i - 1, j], plane[i - 1],
                )
    for j in band_order:
        total = plane_sum[0, j]
        for i in range(1, chips):
            arrivals["plane", i, j].wait_recv()
            total = total + plane_in[i - 1, j]
        band_sum[j] = total
        if j > 0:
            arrivals["band", j] = send(
                band_sum.at[j], band_in.at[j - 1], band_send.at[j - 1], band_recv.at[j - 1],
                column[j - 1],
            )
    total = band_sum[0]
    for j in range(1, bands):
        arrivals["band", j].wait_recv()
        total = total + band_in[j - 1]
    final[...] = total
    arrivals["last"] = send(final, other, last_send, last_recv, mate)
    arrivals["last"].wait_recv()
    theirs = other[...]
    left = jnp.where(core == 0, total, theirs)
    right = jnp.where(core == 0, theirs, total)
    joined = jnp.concatenate([left, right], axis=1)
    height, modes = out_ref.shape
    out_ref[...] = jnp.where(core == 0, joined[:height], joined[height:])[:, :modes]
    for copy in arrivals.values():
        copy.wait_send()


def shards(fields, weights, pair_slots, pair_counts, requests, eofs):
    lat_count, lon_count = lax.axis_size("lat"), lax.axis_size("lon")
    lat_index, lon_index = lax.axis_index("lat"), lax.axis_index("lon")
    device = lat_index * lon_count + lon_index
    grids, src_tiles, cells, columns = fields.shape
    tiles, pairs = weights.shape[1], weights.shape[2]
    modes = eofs.shape[0]
    asked = requests.shape[2]
    up = [(i, (i + 1) % lon_count) for i in range(lon_count)]
    down = [(j, i) for i, j in up]
    smem = pl.BlockSpec(memory_space=pltpu.SMEM)
    vmem = pl.BlockSpec(memory_space=pltpu.VMEM)
    packed = jax.ShapeDtypeStruct((grids, asked // 2, cells, columns), fields.dtype)
    upward, downward = pl.pallas_call(
        pack_kernel, out_shape=[packed, packed], in_specs=[smem, vmem], out_specs=[vmem, vmem],
        compiler_params=pltpu.CompilerParams(vmem_limit_bytes=VMEM_LIMIT),
    )(jnp.transpose(requests, (0, 2, 1)), fields)
    before = lax.ppermute(upward, "lon", up)
    after = lax.ppermute(downward, "lon", down)

    wanted = lax.dynamic_index_in_dim(requests, device, 1, keepdims=False)
    sector = wanted // src_tiles - lat_index * lon_count
    relative = (sector - lon_index + 1 + lon_count) % lon_count
    earlier = jnp.arange(asked)[None, :] < jnp.arange(asked)[:, None]
    same = (relative[:, :, None] == relative[:, None, :]) & earlier
    rank = jnp.sum(same, axis=2, dtype=jnp.int32)
    codes = relative * src_tiles + jnp.where(relative == 1, wanted % src_tiles, rank)
    live = jnp.arange(pairs, dtype=jnp.int32) < pair_counts[:, :, None]
    slots = jnp.where(live, pair_slots, asked).reshape(-1)
    table = jnp.concatenate([slots, codes.reshape(-1)])

    halves = 2
    width = halves * LANES
    block = 4
    while tiles % block:
        block //= 2
    basis = pl.pallas_call(
        functools.partial(basis_kernel, block, tiles),
        out_shape=jax.ShapeDtypeStruct((grids, asked * cells, 3 * width), jnp.bfloat16),
        grid_spec=pltpu.PrefetchScalarGridSpec(
            num_scalar_prefetch=1,
            grid=(tiles // block,),
            in_specs=[
                pl.BlockSpec((grids, block, pairs, cells, TT), lambda s, _: (0, s, 0, 0, 0)),
                pl.BlockSpec((modes, block * TT), lambda s, _: (0, s)),
            ],
            out_specs=pl.BlockSpec((grids, asked * cells, 3 * width), lambda s, _: (0, 0, 0)),
            scratch_shapes=[pltpu.VMEM(((asked + 1) * cells, width), jnp.float32)] * (2 * grids),
        ),
        compiler_params=pltpu.CompilerParams(vmem_limit_bytes=VMEM_LIMIT),
        cost_estimate=pl.CostEstimate(
            flops=2 * weights.size * modes, bytes_accessed=2 * (weights.size + eofs.size),
            transcendentals=0,
        ),
    )(table, weights, eofs)

    chips = lon_count // 2
    rows = grids * columns // (lat_count * chips)
    dma = pltpu.SemaphoreType.DMA
    buffer = lambda *shape: pltpu.VMEM((*shape, rows, LANES), jnp.float32)
    summed = pl.pallas_call(
        reduce_kernel,
        out_shape=jax.ShapeDtypeStruct((rows // 2, modes), jnp.float32),
        in_specs=[smem, vmem, vmem, vmem, vmem],
        out_specs=vmem,
        scratch_shapes=[
            pltpu.VMEM((asked * cells, columns), jnp.bfloat16),
            buffer(halves, chips, lat_count),
            buffer(chips, lat_count), buffer(chips, lat_count), buffer(chips - 1, lat_count),
            buffer(lat_count), buffer(lat_count - 1), buffer(), buffer(),
            dma((chips, lat_count)), dma((chips, lat_count)),
            dma((chips - 1, lat_count)), dma((chips - 1, lat_count)),
            dma((lat_count - 1,)), dma((lat_count - 1,)),
            dma(()), dma(()),
        ],
        compiler_params=pltpu.CompilerParams(
            collective_id=0, has_side_effects=True, vmem_limit_bytes=VMEM_LIMIT
        ),
    )(table, before, fields, after, basis)
    return jnp.transpose(summed)


def solution(mesh):
    return jax.shard_map(
        shards,
        mesh=mesh,
        in_specs=(
            P(None, ("lat", "lon"), None, None),
            P(None, ("lat", "lon"), None, None, None),
            P(None, ("lat", "lon"), None),
            P(None, ("lat", "lon")),
            P(),
            P(None, ("lat", "lon")),
        ),
        out_specs=P(None, ("lat", "lon")),
        check_vma=False,
    )
```
